16 devices in a mesh: rep: 2 (over y, z), dp: 8 (over x, core).
Axes of the slice: x: 4, y: 2, z: 1, core: 2. Of those that a mesh axis runs over, the one named last changes fastest.
The devices are a block of a 4x4x8 slice.
Arguments:
- x: bfloat16 [16, 2048, 1536], P(('rep', 'dp')), parts along dimension 0
- dy: bfloat16 [16, 2048, 1536], P(('rep', 'dp')), parts along dimension 0
- w_gate: bfloat16 [2, 1536, 4224], P(None, 'dp')
- w_up: bfloat16 [2, 1536, 4224], P(None, 'dp')
- w_down: bfloat16 [2, 4224, 1536], P(None, 'dp')
- m_w_gate: float32 [2, 1536, 4224], P(None, 'dp')
- m_w_up: float32 [2, 1536, 4224], P(None, 'dp')
- m_w_down: float32 [2, 4224, 1536], P(None, 'dp')
- v_w_gate: float32 [2, 1536, 4224], P(None, 'dp')
- v_w_up: float32 [2, 1536, 4224], P(None, 'dp')
- v_w_down: float32 [2, 4224, 1536], P(None, 'dp')
Outputs:
- output 1: bfloat16 [4, 1536, 4224], P('rep', 'dp'), parts along dimension 0
- output 2: bfloat16 [4, 1536, 4224], P('rep', 'dp'), parts along dimension 0
- output 3: bfloat16 [4, 4224, 1536], P('rep', 'dp'), parts along dimension 0
- output 4: float32 [4, 1536, 4224], P('rep', 'dp'), parts along dimension 0
- output 5: float32 [4, 1536, 4224], P('rep', 'dp'), parts along dimension 0
- output 6: float32 [4, 4224, 1536], P('rep', 'dp'), parts along dimension 0
- output 7: float32 [4, 1536, 4224], P('rep', 'dp'), parts along dimension 0
- output 8: float32 [4, 1536, 4224], P('rep', 'dp'), parts along dimension 0
- output 9: float32 [4, 4224, 1536], P('rep', 'dp'), parts along dimension 0
There are 2 independent parts. The reference program is written for one: setup_inputs(seed, part) draws one part's arguments, and reference() takes and returns one part's arrays. A program takes and returns all parts, laid end to end along the dimension named above; an argument that names none is the same for every part.
All inputs are finite; a program needn't handle non-finite values.
Results may differ from the reference program's by a relative error of at most 0.022.
Values are sent between devices in bfloat16 or wider.
A program may use at most 768 MiB of HBM per device.

```python
import jax
import jax.numpy as jnp
from jax import lax

SEQUENCES = 8
TOKENS = 2048
D = 1536
FF = 4224
LAYERS = 2
NAMES = ("w_gate", "w_up", "w_down")
SHAPES = {"w_gate": (LAYERS, D, FF), "w_up": (LAYERS, D, FF), "w_down": (LAYERS, FF, D)}


def bump(key, n, height):
    away = (jnp.arange(n, dtype=jnp.int32) - jax.random.randint(key, (), 0, n, jnp.int32)) % n
    return jnp.where(away < n // 8, height, 1.0)


def together(key, own, strength):
    shared = jax.random.normal(key, own.shape[1:], jnp.float32)
    return (own + strength * shared) * lax.rsqrt(1 + strength * strength)


def setup_inputs(seed: int = 0, part: int = 0) -> dict:
    kx, kdy, ka, kb, kz, kf, kh, kl, *keys = jax.random.split(jax.random.key(seed), 8 + 3 * len(NAMES))
    kx, kdy, ka, kb = (jax.random.fold_in(k, part) for k in (kx, kdy, ka, kb))
    kw, km, kv = (keys[i::3] for i in range(3))
    shape = (SEQUENCES, TOKENS, D)
    much_x, much_dy = jax.random.uniform(kz, (2,), jnp.float32, 0.0, 1.0)
    loud = 2.0 ** jax.random.uniform(jax.random.fold_in(kz, 1), (), jnp.float32, -1.0, 2.0)
    layers = 2.0 ** jax.random.uniform(kl, (LAYERS, 1, 1), jnp.float32, -1.0, 1.0)
    x = together(ka, jax.random.normal(kx, shape, jnp.float32), much_x) * bump(kf, D, 4.0)
    dy = together(kb, jax.random.normal(kdy, shape, jnp.float32), much_dy)
    drawn = {"x": x.astype(jnp.bfloat16), "dy": (loud * dy * (SEQUENCES * TOKENS) ** -0.5).astype(jnp.bfloat16)}
    for key, name in zip(kw, NAMES, strict=True):
        w = jax.random.normal(key, SHAPES[name], jnp.float32) * SHAPES[name][1] ** -0.5
        drawn[name] = (w * {"w_gate": 1.0, "w_up": bump(kh, FF, 4.0), "w_down": layers}[name]).astype(jnp.bfloat16)
    for key, name in zip(km, NAMES, strict=True):
        drawn[f"m_{name}"] = 0.1 * jax.random.normal(key, SHAPES[name], jnp.float32)
    for key, name in zip(kv, NAMES, strict=True):
        drawn[f"v_{name}"] = jax.random.uniform(key, SHAPES[name], jnp.float32, 0.005, 0.015)
    return drawn


def matmul(a, w):
    return jnp.dot(a, w, preferred_element_type=jnp.float32).astype(jnp.bfloat16)


def normed(h):
    wide = h.astype(jnp.float32)
    scale = lax.rsqrt(jnp.mean(wide**2, -1, keepdims=True) + 1e-6)
    return (wide * scale).astype(jnp.bfloat16)


def layer(h, w):
    a = normed(h)
    gate = jnp.dot(a, w["w_gate"], preferred_element_type=jnp.float32)
    up = jnp.dot(a, w["w_up"], preferred_element_type=jnp.float32)
    return h + matmul((jax.nn.silu(gate) * up).astype(jnp.bfloat16), w["w_down"])


def adamw(w, m, v, g):
    m = 0.9 * m + 0.1 * g
    v = 0.95 * v + 0.05 * g * g
    step = m * lax.rsqrt(v + 1e-8) + 0.1 * w
    return (w - 0.02 * step).astype(jnp.bfloat16), m, v


def clipped(gradients, sum_of_squares, count):
    factor = jnp.minimum(1.0, 0.5 * lax.rsqrt(sum_of_squares / count + 1e-30))
    return [g * factor for g in gradients]


def stack(weights, h):
    return lax.scan(lambda h, w: (layer(h, w), None), h, weights)[0]


def reference(x, dy, w_gate, w_up, w_down, m_w_gate, m_w_up, m_w_down, v_w_gate, v_w_up, v_w_down):
    weights = dict(zip(NAMES, (w_gate, w_up, w_down), strict=True))

    def take(so_far, sequence):
        h, by_y = sequence
        _, back = jax.vjp(lambda w: stack(w, h), weights)
        return jax.tree.map(lambda total, term: total + term.astype(jnp.float32), so_far, back(by_y)[0]), None

    none_yet = {name: jnp.zeros(w.shape, jnp.float32) for name, w in weights.items()}
    by_weights, _ = lax.scan(take, none_yet, (x, dy))
    gradients = [by_weights[name].astype(jnp.bfloat16).astype(jnp.float32) for name in NAMES]
    gradients = clipped(gradients, sum(jnp.sum(g * g) for g in gradients), sum(g.size for g in gradients))
    new = [
        adamw(w.astype(jnp.float32), m, v, g)
        for w, m, v, g in zip((w_gate, w_up, w_down), (m_w_gate, m_w_up, m_w_down), (v_w_gate, v_w_up, v_w_down), gradients, strict=True)
    ]
    return tuple(one[which] for which in range(3) for one in new)
```

```python
import functools
import jax, jax.numpy as jnp
from jax import lax
from jax.experimental import pallas as pl
from jax.experimental.pallas import tpu as pltpu
from jax.sharding import PartitionSpec as P
MESH=pl.DeviceIdType.MESH
BF, F32 = jnp.bfloat16, jnp.float32
VMEM_LIMIT = 67043328

def norm_of(wide):
    return (wide * lax.rsqrt(jnp.mean(wide * wide, -1, keepdims=True) + 1e-6)).astype(BF)

TN = 256
TB = 512
CH = 512

def fwd_kernel(n, x, wg, wu, wd, WG, WU, WD, GATE, UP, HIDT, AT, H1,
               a_v, wbuf, wtail, gbuf, ubuf, hbuf, gtail, utail, htail, wd_v, htbuf, xbuf, h1buf, atbuf, bounce, bounced,
               send, recv, w_sem, g_sem, u_sem, h_sem, wd_sem, ht_sem, x_sem, h1_sem, at_sem, b_sem, b_out):
    T, D = x.shape
    F = wg.shape[2]
    full = F // TN
    rest = F - full * TN
    r, me = lax.axis_index("rep"), lax.axis_index("dp")
    right, left = lax.rem(me + 2, n), lax.rem(me + n - 2, n)
    across = lax.rem(me + n // 2, n)
    odd = lax.rem(me, 2)
    sib = me + 1 - 2 * odd
    par = lax.rem(r, 2)
    partner = r + 1 - 2 * par
    to = {"R": (r, right), "L": (r, left), "S": (r, sib), "Y": (partner, me)}

    def twin(d):
        return d + 1 - 2 * odd

    shards = [(wg, WG, 0), (wu, WU, 0), (wd, WD, 0), (wg, WG, 1), (wu, WU, 1), (wd, WD, 1)]

    def moves(m):
        w, W, l = shards[m]
        R = w.shape[1]
        c = R // 3
        N, P1, P2, ALL = (0, c), (c * (1 + par), c), (c * (2 - par), c), (0, R)
        return {
            "rN": (me, N, "R", True), "lP": (me, P1, "L", True), "rP": (me, P1, "R", True), "lN": (me, N, "L", True),
            "sO": (me, ALL, "S", True),
            "oN": (left, N, "R", False), "oP": (right, P1, "L", False),
            "ylP": (right, P1, "Y", False), "yrP": (left, P1, "Y", False), "yoP": (across, P1, "Y", False),
            "srN": (left, N, "S", False), "srP": (left, P1, "S", False), "slP": (right, P1, "S", False), "slN": (right, N, "S", False),
            "soN": (across, N, "S", False), "soP": (across, P1, "S", False),
            "syl": (right, P2, "S", False), "syr": (left, P2, "S", False), "syo": (across, P2, "S", False),
        }

    ORDER = list(moves(0))

    def copy(m, name):
        w, W, l = shards[m]
        R = w.shape[1]
        owner, (first, rows), way, own = moves(m)[name]
        there = W.at[l, pl.ds(pl.multiple_of(owner * R + first, 8), rows)]
        src = w.at[l, pl.ds(pl.multiple_of(first, 8) if not isinstance(first, int) else first, rows)] if own else there
        k = ORDER.index(name)
        return pltpu.make_async_remote_copy(src_ref=src, dst_ref=there, send_sem=send.at[m, k], recv_sem=recv.at[m, k],
                                            device_id=to[way], device_id_type=MESH)

    def start(m, *names):
        for name in names:
            copy(m, name).start()

    def arrive(m, *names):
        for name in names:
            copy(m, name).wait_recv()

    def e1(m): start(m, "rN", "lP", "rP", "lN", "sO")
    def e2(m):
        arrive(m, "rN", "lP"); start(m, "oN", "oP", "ylP", "srN", "slP")
    def e3(m):
        arrive(m, "rP", "lN"); start(m, "yrP", "srP", "slN")
    def e4(m):
        arrive(m, "oN", "oP", "ylP"); start(m, "yoP", "soN", "soP", "syl")
    def e5(m):
        arrive(m, "yrP"); start(m, "syr")
    def e6(m):
        arrive(m, "yoP"); start(m, "syo")
    def e7(m):
        arrive(m, "sO", "srN", "srP", "slP", "slN", "soN", "soP", "syl", "syr", "syo")

    M = len(shards)
    def tick(t):
        m, phase = divmod(t, 3)
        if phase == 0:
            if 0 <= m - 1 < M: e4(m - 1); e5(m - 1)
        elif phase == 1:
            if m < M: e2(m)
            if 0 <= m - 1 < M: e6(m - 1)
        else:
            if m < M: e3(m)
            if m + 1 < M: e1(m + 1)

    barrier = pltpu.get_barrier_semaphore()
    for way in to:
        pl.semaphore_signal(barrier, inc=1, device_id=to[way], device_id_type=MESH)
    pl.semaphore_wait(barrier, 4)
    e1(0)

    def slot_of(m):
        w, W, l = shards[m]
        return bounced if w is wd else bounce
    def own_in(m):
        w, W, l = shards[m]
        return pltpu.make_async_copy(w.at[l], slot_of(m), b_sem.at[m])
    def own_out(m):
        w, W, l = shards[m]
        R = w.shape[1]
        return pltpu.make_async_copy(slot_of(m), W.at[l, pl.ds(pl.multiple_of(me * R, 8), R)], b_out.at[m])
    own_in(0).start(); own_in(2).start()

    nb = T // TB
    def x_in(i, s): return pltpu.make_async_copy(x.at[pl.ds(i * TB, TB)], xbuf.at[s], x_sem.at[s])
    def at_out(l, i, s): return pltpu.make_async_copy(atbuf.at[s], AT.at[l, :, pl.ds(i * TB, TB)], at_sem.at[s])
    def h1_out(i, s): return pltpu.make_async_copy(h1buf.at[s], H1.at[pl.ds(i * TB, TB)], h1_sem.at[s])
    def put_a(l, i, s, wide):
        a = norm_of(wide)
        a_v[pl.ds(i * TB, TB)] = a
        atbuf[s] = a.T
        at_out(l, i, s).start()
    x_in(0, 0).start()
    for i in range(nb):
        s = i % 2
        x_in(i, s).wait()
        if i + 1 < nb: x_in(i + 1, 1 - s).start()
        if i >= 2: at_out(0, i - 2, s).wait()
        put_a(0, i, s, xbuf[s].astype(F32))
    for i in (nb - 2, nb - 1): at_out(0, i, i % 2).wait()
    own_in(2).wait(); own_out(2).start()
    for m, after in ((0, 1), (1, 3), (3, 4), (4, None)):
        own_in(m).wait(); own_out(m).start(); own_out(m).wait()
        if after is not None: own_in(after).start()
        if m == 0:
            own_out(2).wait(); own_in(5).start()
    own_in(5).wait(); own_out(5).start(); own_out(5).wait()

    for t in (1, 2, 3, 4): tick(t)

    def cols(j): return pl.ds(pl.multiple_of(j * TN, TN), TN)
    LAST = pl.ds(full * TN, rest)

    def columns_phase(W, l, up, ticks):
        def w_in(j, s): return pltpu.make_async_copy(W.at[l, :, cols(j)], wbuf.at[s], w_sem.at[s])
        def w_in_last(): return pltpu.make_async_copy(W.at[l, :, LAST], wtail, w_sem.at[2])
        def g_in(j, s): return pltpu.make_async_copy(GATE.at[l, :, cols(j)], gbuf.at[s], g_sem.at[s])
        def g_in_last(): return pltpu.make_async_copy(GATE.at[l, :, LAST], gtail, g_sem.at[2])
        def g_out(j, s): return pltpu.make_async_copy(gbuf.at[s], GATE.at[l, :, cols(j)], g_sem.at[s])
        def g_out_last(): return pltpu.make_async_copy(gtail, GATE.at[l, :, LAST], g_sem.at[2])
        def u_out(j, s): return pltpu.make_async_copy(ubuf.at[s], UP.at[l, :, cols(j)], u_sem.at[s])
        def u_out_last(): return pltpu.make_async_copy(utail, UP.at[l, :, LAST], u_sem.at[2])
        def h_out(j, s): return pltpu.make_async_copy(hbuf.at[s], HIDT.at[l, cols(j)], h_sem.at[s])
        def h_out_last(): return pltpu.make_async_copy(htail, HIDT.at[l, LAST], h_sem.at[2])

        def compute(w_ref, g_ref, u_ref, h_ref):
            for c in range(T // CH):
                rows = pl.ds(c * CH, CH)
                got = jnp.dot(a_v[rows], w_ref[...], preferred_element_type=F32)
                if not up:
                    g_ref[rows] = got
                else:
                    g = g_ref[rows]
                    u_ref[rows] = got
                    hid = (g * (1 / (1 + jnp.exp(-g))) * got).astype(BF)
                    h_ref[:, rows] = hid.T

        w_in(0, 0).start()
        if up: g_in(0, 0).start()
        def step(j, carry):
            s = lax.rem(j, 2)
            for at, t in ticks.items():
                if at < full:
                    @pl.when(j == at)
                    def _(): tick(t)
            w_in(j, s).wait()
            if up: g_in(j, s).wait()
            @pl.when(j + 1 < full)
            def _():
                w_in(j + 1, 1 - s).start()
                if up: g_in(j + 1, 1 - s).start()
            @pl.when(j + 1 == full)
            def _():
                w_in_last().start()
                if up: g_in_last().start()
            @pl.when(j >= 2)
            def _():
                if up:
                    u_out(j - 2, s).wait(); h_out(j - 2, s).wait()
                else:
                    g_out(j - 2, s).wait()
            compute(wbuf.at[s], gbuf.at[s], ubuf.at[s], hbuf.at[s])
            if up:
                u_out(j, s).start(); h_out(j, s).start()
            else:
                g_out(j, s).start()
            return carry
        lax.fori_loop(0, full, step, 0)
        w_in_last().wait()
        if up: g_in_last().wait()
        compute(wtail, gtail, utail, htail)
        if up:
            u_out_last().start(); h_out_last().start()
        else:
            g_out_last().start()
        for at, t in ticks.items():
            if at >= full: tick(t)
        for j in (full - 2, full - 1):
            if up:
                u_out(j, j % 2).wait(); h_out(j, j % 2).wait()
            else:
                g_out(j, j % 2).wait()
        if up:
            u_out_last().wait(); h_out_last().wait()
        else:
            g_out_last().wait()

    def down_phase(ticks):
        wd_in = pltpu.make_async_copy(WD.at[0], wd_v, wd_sem)
        wd_in.start()
        def ht_in(i, s): return pltpu.make_async_copy(HIDT.at[0, :, pl.ds(pl.multiple_of(i * TB, TB), TB)], htbuf.at[s], ht_sem.at[s])
        ht_in(0, 0).start(); x_in(0, 0).start()
        wd_in.wait()
        def step(i, carry):
            s = lax.rem(i, 2)
            for at, t in ticks.items():
                if at < nb:
                    @pl.when(i == at)
                    def _(): tick(t)
            ht_in(i, s).wait(); x_in(i, s).wait()
            @pl.when(i + 1 < nb)
            def _():
                ht_in(i + 1, 1 - s).start(); x_in(i + 1, 1 - s).start()
            @pl.when(i >= 2)
            def _():
                at_out(1, i - 2, s).wait(); h1_out(i - 2, s).wait()
            got = lax.dot_general(htbuf[s], wd_v[...], (((0,), (0,)), ((), ())), preferred_element_type=F32).astype(BF)
            h1 = (xbuf[s].astype(F32) + got.astype(F32)).astype(BF)
            h1buf[s] = h1
            h1_out(i, s).start()
            put_a(1, i, s, h1.astype(F32))
            return carry
        lax.fori_loop(0, nb, step, 0)
        for at, t in ticks.items():
            if at >= nb: tick(t)
        for i in (nb - 2, nb - 1):
            at_out(1, i, i % 2).wait(); h1_out(i, i % 2).wait()

    e7(0)
    columns_phase(WG, 0, False, {4: 5, 10: 6, 99: 7})
    e7(1)
    columns_phase(WU, 0, True, {4: 8, 10: 9, 99: 10})
    e7(2)
    down_phase({1: 11, 2: 12, 99: 13})
    e7(3)
    columns_phase(WG, 1, False, {4: 14, 10: 15, 99: 16})
    e7(4)
    columns_phase(WU, 1, True, {4: 17, 10: 18, 99: 19})
    e7(5)
    for m in range(M):
        for name in ORDER: copy(m, name).wait_send()

def fwd(n, x, wg, wu, wd):
    T, D = x.shape
    L, RG, F = wg.shape
    RD = wd.shape[1]
    rest = F % TN
    S = jax.ShapeDtypeStruct
    A = pl.BlockSpec(memory_space=pl.ANY)
    DMA = pltpu.SemaphoreType.DMA
    V = pltpu.VMEM
    return pl.pallas_call(
        functools.partial(fwd_kernel, n),
        out_shape=[S((L, D, F), BF), S((L, D, F), BF), S((L, F, D), BF), S((L, T, F), F32), S((L, T, F), F32), S((L, F, T), BF), S((L, D, T), BF), S((T, D), BF)],
        in_specs=[A] * 4, out_specs=[A] * 8,
        scratch_shapes=[
            V((T, D), BF), V((2, D, TN), BF), V((D, rest), BF), V((2, T, TN), F32), V((2, T, TN), F32), V((2, TN, T), BF),
            V((T, rest), F32), V((T, rest), F32), V((rest, T), BF), V((F, D), BF), V((2, F, TB), BF), V((2, TB, D), BF), V((2, TB, D), BF), V((2, D, TB), BF),
            V((RG, F), BF), V((RD, D), BF),
            DMA((6, 19)), DMA((6, 19)), DMA((3,)), DMA((3,)), DMA((3,)), DMA((3,)), DMA(()), DMA((2,)), DMA((2,)), DMA((2,)), DMA((2,)), DMA((6,)), DMA((6,)),
        ],
        compiler_params=pltpu.CompilerParams(collective_id=0, has_side_effects=True, vmem_limit_bytes=VMEM_LIMIT),
        name="forward",
    )(x, wg, wu, wd)


def adamw(w, m, v, g):
    m = 0.9 * m + 0.1 * g
    v = 0.95 * v + 0.05 * g * g
    step = m * lax.rsqrt(v + 1e-8) + 0.1 * w
    return (w - 0.02 * step).astype(BF), m, v


def matmul(a, b, over):
    return lax.dot_general(a, b, (((over[0],), (over[1],)), ((), ())), preferred_element_type=F32).astype(BF)


def normed(h):
    return norm_of(h.astype(F32))


def solution(mesh):
    n = mesh.shape["dp"]

    def step(x, dy, *arrays):
        weights, m, v = (arrays[i : i + 3] for i in (0, 3, 6))
        layers = weights[0].shape[0]
        h0, by_h = x[0], dy[0]
        WG, WU, WD, GATE, UP, HIDT, AT, H1 = fwd(n, h0, *weights)
        kept, mine = (h0, H1), [None] * layers
        def scattered(g):
            return lax.psum_scatter(g, "dp", scatter_dimension=0, tiled=True)
        for l in reversed(range(layers)):
            gate, up = GATE[l], UP[l]
            down = scattered(matmul(HIDT[l], by_h, (1, 0)))
            by_hid = matmul(by_h, WD[l], (1, 1)).astype(F32)
            sig = jax.nn.sigmoid(gate)
            by_up = (by_hid * gate * sig).astype(BF)
            by_gate = (by_hid * up * sig * (1 + gate * (1 - sig))).astype(BF)
            mine[l] = [scattered(matmul(AT[l], by_gate, (1, 0))), scattered(matmul(AT[l], by_up, (1, 0))), down]
            if l:
                by_a = matmul(by_gate, WG[l], (1, 1)) + matmul(by_up, WU[l], (1, 1))
                by_h = by_h + jax.vjp(normed, kept[l])[1](by_a)[0]
        gradients = [jnp.stack([mine[number][i] for number in range(layers)]).astype(F32) for i in range(3)]
        squares = lax.psum(sum(jnp.sum(g * g) for g in gradients), "dp")
        count = lax.psum(1, "dp") * sum(g.size for g in gradients)
        factor = jnp.minimum(1.0, 0.5 * lax.rsqrt(squares / count + 1e-30))
        new = [adamw(w.astype(F32), m, v, g * factor) for w, m, v, g in zip(weights, m, v, gradients, strict=True)]
        return tuple(one[which] for which in range(3) for one in new)

    states, cut = P(("rep", "dp"), None, None), P(None, "dp", None)
    return jax.shard_map(step, mesh=mesh, in_specs=(states, states) + (cut,) * 9, out_specs=(P("rep", "dp", None),) * 9, check_vma=False)
```

```python
import functools
import jax, jax.numpy as jnp
from jax import lax
from jax.experimental import pallas as pl
from jax.experimental.pallas import tpu as pltpu
from jax.sharding import PartitionSpec as P
ZERO, ONE, TWO = range(3)
MESH=pl.DeviceIdType.MESH
BF, F32 = jnp.bfloat16, jnp.float32
VMEM_LIMIT = 67043328

def norm_of(wide):
    return (wide * lax.rsqrt(jnp.mean(wide * wide, -ONE, keepdims=True) + 1e-6)).astype(BF)

TN = 256
TD = 256
TB = 512
CH = 512

def fwd_kernel(n, x, wg, wu, wd, WG, WU, WD, GATE, UP, HIDT, AT, H1, WGT, WUT,
               a_v, xbuf, atbuf,
               send, recv, w_sem, g_sem, go_sem, u_sem, h_sem, t_sem, wd_sem, ht_sem, x_sem, h1_sem, at_sem, b_sem, b_out):
    T, D = x.shape
    F = wg.shape[TWO]
    full = F // TN
    rest = F - full * TN
    r, me = lax.axis_index("rep"), lax.axis_index("dp")
    right, left = lax.rem(me + TWO, n), lax.rem(me + n - TWO, n)
    across = lax.rem(me + n // TWO, n)
    odd = lax.rem(me, TWO)
    sib = me + ONE - TWO * odd
    par = lax.rem(r, TWO)
    partner = r + ONE - TWO * par
    to = {"R": (r, right), "L": (r, left), "S": (r, sib), "Y": (partner, me)}

    def twin(d):
        return d + ONE - TWO * odd

    shards = [(wg, WG, ZERO), (wu, WU, ZERO), (wd, WD, ZERO), (wg, WG, ONE), (wu, WU, ONE), (wd, WD, ONE)]

    def moves(m):
        w, W, l = shards[m]
        R = w.shape[ONE]
        c = R // 3
        N, P1, P2, ALL = (ZERO, c), (c * (ONE + par), c), (c * (TWO - par), c), (ZERO, R)
        return {
            "rN": (me, N, "R", True), "lP": (me, P1, "L", True), "rP": (me, P1, "R", True), "lN": (me, N, "L", True),
            "sO": (me, ALL, "S", True),
            "oN": (left, N, "R", False), "oP": (right, P1, "L", False),
            "ylP": (right, P1, "Y", False), "yrP": (left, P1, "Y", False), "yoP": (across, P1, "Y", False),
            "srN": (left, N, "S", False), "srP": (left, P1, "S", False), "slP": (right, P1, "S", False), "slN": (right, N, "S", False),
            "soN": (across, N, "S", False), "soP": (across, P1, "S", False),
            "syl": (right, P2, "S", False), "syr": (left, P2, "S", False), "syo": (across, P2, "S", False),
        }

    ORDER = list(moves(ZERO))

    def copy(m, name):
        w, W, l = shards[m]
        R = w.shape[ONE]
        owner, (first, rows), way, own = moves(m)[name]
        there = W.at[l, pl.ds(pl.multiple_of(owner * R + first, 8), rows)]
        src = w.at[l, pl.ds(pl.multiple_of(first, 8) if not isinstance(first, int) else first, rows)] if own else there
        k = ORDER.index(name)
        return pltpu.make_async_remote_copy(src_ref=src, dst_ref=there, send_sem=send.at[m, k], recv_sem=recv.at[m, k],
                                            device_id=to[way], device_id_type=MESH)

    def start(m, *names):
        for name in names:
            copy(m, name).start()

    def arrive(m, *names):
        for name in names:
            copy(m, name).wait_recv()

    def e1(m): start(m, "rN", "lP", "rP", "lN", "sO")
    def e2(m):
        arrive(m, "rN", "lP"); start(m, "oN", "oP", "ylP", "srN", "slP")
    def e3(m):
        arrive(m, "rP", "lN"); start(m, "yrP", "srP", "slN")
    def e4(m):
        arrive(m, "oN", "oP", "ylP"); start(m, "yoP", "soN", "soP", "syl")
    def e5(m):
        arrive(m, "yrP"); start(m, "syr")
    def e6(m):
        arrive(m, "yoP"); start(m, "syo")
    def e7(m):
        arrive(m, "sO", "srN", "srP", "slP", "slN", "soN", "soP", "syl", "syr", "syo")

    M = len(shards)
    def tick(t):
        m, phase = divmod(t, 3)
        if phase == ZERO:
            if ZERO <= m - ONE < M: e4(m - ONE); e5(m - ONE)
        elif phase == ONE:
            if m < M: e2(m)
            if ZERO <= m - ONE < M: e6(m - ONE)
        else:
            if m < M: e3(m)
            if m + ONE < M: e1(m + ONE)

    barrier = pltpu.get_barrier_semaphore()
    for way in to:
        pl.semaphore_signal(barrier, inc=ONE, device_id=to[way], device_id_type=MESH)
    pl.semaphore_wait(barrier, 4)
    e1(ZERO)

    nb = T // TB
    def x_in(i, s): return pltpu.make_async_copy(x.at[pl.ds(i * TB, TB)], xbuf.at[s], x_sem.at[s])
    def at_out(l, i, s): return pltpu.make_async_copy(atbuf.at[s], AT.at[l, :, pl.ds(i * TB, TB)], at_sem.at[s])
    def put_a(l, i, s, wide):
        a = norm_of(wide)
        a_v[pl.ds(i * TB, TB)] = a
        atbuf[s] = a.T
        at_out(l, i, s).start()
    def settle_own(bounce, bounced):
        def slot_of(m):
            return bounced if shards[m][ZERO] is wd else bounce
        def own_in(m):
            w, W, l = shards[m]
            return pltpu.make_async_copy(w.at[l], slot_of(m), b_sem.at[m])
        def own_out(m):
            w, W, l = shards[m]
            R = w.shape[ONE]
            return pltpu.make_async_copy(slot_of(m), W.at[l, pl.ds(pl.multiple_of(me * R, 8), R)], b_out.at[m])
        own_in(ZERO).start(); own_in(TWO).start()
        x_in(ZERO, ZERO).start()
        for i in range(nb):
            s = i % TWO
            x_in(i, s).wait()
            if i + ONE < nb: x_in(i + ONE, ONE - s).start()
            if i >= TWO: at_out(ZERO, i - TWO, s).wait()
            put_a(ZERO, i, s, xbuf[s].astype(F32))
        for i in (nb - TWO, nb - ONE): at_out(ZERO, i, i % TWO).wait()
        own_in(TWO).wait(); own_out(TWO).start()
        for m, after in ((ZERO, ONE), (ONE, 3), (3, 4), (4, None)):
            own_in(m).wait(); own_out(m).start(); own_out(m).wait()
            if after is not None: own_in(after).start()
            if m == ZERO:
                own_out(TWO).wait(); own_in(5).start()
        own_in(5).wait(); own_out(5).start(); own_out(5).wait()
    pl.run_scoped(settle_own, pltpu.VMEM(wg.shape[ONE:], BF), pltpu.VMEM(wd.shape[ONE:], BF))

    for t in (ONE, TWO, 3, 4): tick(t)

    def cols(j): return pl.ds(pl.multiple_of(j * TN, TN), TN)
    LAST = pl.ds(full * TN, rest)

    def columns_phase(W, WT, l, up, ticks):
        turn = WT is not None
        def body(wbuf, gbuf, ubuf, hbuf, tbuf, wtail, gtail, utail, htail, ttail):
            LASTC = (full, slice(None), pl.ds(ZERO, rest))
            def ins(j, s):
                got = [pltpu.make_async_copy(W.at[l, :, cols(j)], wbuf.at[s], w_sem.at[s])]
                if up: got.append(pltpu.make_async_copy(GATE.at[l, j], gbuf.at[s], g_sem.at[s]))
                return got
            def ins_last():
                got = [pltpu.make_async_copy(W.at[l, :, LAST], wtail, w_sem.at[3])]
                if up: got.append(pltpu.make_async_copy(GATE.at[l, full, :, pl.ds(ZERO, rest)], gtail, g_sem.at[3]))
                return got
            def outs(j, s):
                if up:
                    got = [pltpu.make_async_copy(ubuf.at[s], UP.at[l, j], u_sem.at[s]), pltpu.make_async_copy(hbuf.at[s], HIDT.at[l, cols(j)], h_sem.at[s])]
                else:
                    got = [pltpu.make_async_copy(gbuf.at[s], GATE.at[l, j], go_sem.at[s])]
                if turn: got.append(pltpu.make_async_copy(tbuf.at[s], WT.at[:, cols(j)], t_sem.at[s]))
                return got
            def outs_last():
                if up:
                    got = [pltpu.make_async_copy(utail, UP.at[l, full, :, pl.ds(ZERO, rest)], u_sem.at[TWO]), pltpu.make_async_copy(htail, HIDT.at[l, LAST], h_sem.at[TWO])]
                else:
                    got = [pltpu.make_async_copy(gtail, GATE.at[l, full, :, pl.ds(ZERO, rest)], go_sem.at[TWO])]
                if turn: got.append(pltpu.make_async_copy(ttail, WT.at[:, LAST], t_sem.at[TWO]))
                return got
            def compute(w_ref, g_ref, u_ref, h_ref, t_ref):
                for c in range(T // CH):
                    rows = pl.ds(c * CH, CH)
                    got = jnp.dot(a_v[rows], w_ref[...], preferred_element_type=F32)
                    if not up:
                        g_ref[rows] = got
                    else:
                        g = g_ref[rows]
                        u_ref[rows] = got
                        hid = (g * (ONE / (ONE + jnp.exp(-g))) * got).astype(BF)
                        h_ref[:, rows] = hid.T
                if turn:
                    for d in range(D // TD):
                        t_ref[d] = w_ref[d * TD:(d + ONE) * TD].T
            for j in (ZERO, ONE):
                for c in ins(j, j): c.start()
            def step(j, carry):
                s, o = lax.rem(j, 3), lax.rem(j, TWO)
                for at, t in ticks.items():
                    if at < full:
                        @pl.when(j == at)
                        def _(): tick(t)
                for c in ins(j, s): c.wait()
                @pl.when(j + TWO < full)
                def _():
                    for c in ins(j + TWO, lax.rem(j + TWO, 3)): c.start()
                @pl.when(j + TWO == full)
                def _():
                    for c in ins_last(): c.start()
                @pl.when(j >= TWO)
                def _():
                    for c in outs(j - TWO, o): c.wait()
                compute(wbuf.at[s], gbuf.at[s] if up else gbuf.at[o], ubuf.at[o], hbuf.at[o], tbuf.at[o])
                for c in outs(j, o): c.start()
                return carry
            lax.fori_loop(ZERO, full, step, ZERO)
            for c in ins_last(): c.wait()
            compute(wtail, gtail, utail, htail, ttail)
            for c in outs_last(): c.start()
            for at, t in ticks.items():
                if at >= full: tick(t)
            for j in (full - TWO, full - ONE):
                for c in outs(j, j % TWO): c.wait()
            for c in outs_last(): c.wait()
        V = pltpu.VMEM
        nd = D // TD
        pl.run_scoped(body, V((3, D, TN), BF), V((3, T, TN), F32), V((TWO, T, TN) if up else (TWO, 8, 128), F32), V((TWO, TN, T) if up else (TWO, 8, 128), BF),
                      V((TWO, nd, TN, TD) if turn else (TWO, 8, 128), BF), V((D, rest), BF), V((T, rest), F32), V((T, rest), F32), V((rest, T), BF), V((nd, rest, TD), BF))

    def down_phase(ticks):
        def body(wd_v, htbuf, h1buf):
            def h1_out(i, s): return pltpu.make_async_copy(h1buf.at[s], H1.at[pl.ds(i * TB, TB)], h1_sem.at[s])
            wd_in = pltpu.make_async_copy(WD.at[ZERO], wd_v, wd_sem)
            wd_in.start()
            def ht_in(i, s): return pltpu.make_async_copy(HIDT.at[ZERO, :, pl.ds(pl.multiple_of(i * TB, TB), TB)], htbuf.at[s], ht_sem.at[s])
            ht_in(ZERO, ZERO).start(); x_in(ZERO, ZERO).start()
            wd_in.wait()
            def step(i, carry):
                s = lax.rem(i, TWO)
                for at, t in ticks.items():
                    if at < nb:
                        @pl.when(i == at)
                        def _(): tick(t)
                ht_in(i, s).wait(); x_in(i, s).wait()
                @pl.when(i + ONE < nb)
                def _():
                    ht_in(i + ONE, ONE - s).start(); x_in(i + ONE, ONE - s).start()
                @pl.when(i >= TWO)
                def _():
                    at_out(ONE, i - TWO, s).wait(); h1_out(i - TWO, s).wait()
                got = lax.dot_general(htbuf[s], wd_v[...], (((ZERO,), (ZERO,)), ((), ())), preferred_element_type=F32).astype(BF)
                h1 = (xbuf[s].astype(F32) + got.astype(F32)).astype(BF)
                h1buf[s] = h1
                h1_out(i, s).start()
                put_a(ONE, i, s, h1.astype(F32))
                return carry
            lax.fori_loop(ZERO, nb, step, ZERO)
            for at, t in ticks.items():
                if at >= nb: tick(t)
            for i in (nb - TWO, nb - ONE):
                at_out(ONE, i, i % TWO).wait(); h1_out(i, i % TWO).wait()
        pl.run_scoped(body, pltpu.VMEM((F, D), BF), pltpu.VMEM((TWO, F, TB), BF), pltpu.VMEM((TWO, TB, D), BF))

    e7(ZERO)
    columns_phase(WG, None, ZERO, False, {4: 5, 10: 6, 99: 7})
    e7(ONE)
    columns_phase(WU, None, ZERO, True, {4: 8, 10: 9, 99: 10})
    e7(TWO)
    down_phase({ONE: 11, TWO: 12, 99: 13})
    e7(3)
    columns_phase(WG, WGT, ONE, False, {4: 14, 10: 15, 99: 16})
    e7(4)
    columns_phase(WU, WUT, ONE, True, {4: 17, 10: 18, 99: 19})
    e7(5)
    for m in range(M):
        for name in ORDER: copy(m, name).wait_send()

def fwd(n, x, wg, wu, wd):
    T, D = x.shape
    L, RG, F = wg.shape
    RD = wd.shape[ONE]
    steps = pl.cdiv(F, TN)
    S = jax.ShapeDtypeStruct
    A = pl.BlockSpec(memory_space=pl.ANY)
    DMA = pltpu.SemaphoreType.DMA
    V = pltpu.VMEM
    return pl.pallas_call(
        functools.partial(fwd_kernel, n),
        out_shape=[S((L, D, F), BF), S((L, D, F), BF), S((L, F, D), BF), S((L, steps, T, TN), F32), S((L, steps, T, TN), F32), S((L, F, T), BF), S((L, D, T), BF), S((T, D), BF),
                   S((D // TD, F, TD), BF), S((D // TD, F, TD), BF)],
        in_specs=[A] * 4, out_specs=[A] * 10,
        scratch_shapes=[
            V((T, D), BF), V((TWO, TB, D), BF), V((TWO, D, TB), BF),
            DMA((6, 19)), DMA((6, 19)), DMA((4,)), DMA((4,)), DMA((3,)), DMA((3,)), DMA((3,)), DMA((3,)), DMA(()), DMA((TWO,)), DMA((TWO,)), DMA((TWO,)), DMA((TWO,)), DMA((6,)), DMA((6,)),
        ],
        compiler_params=pltpu.CompilerParams(collective_id=ZERO, has_side_effects=True, vmem_limit_bytes=VMEM_LIMIT),
        name="forward",
    )(x, wg, wu, wd)


class Chunk:
    def __init__(self, kind, mi, first, width, number):
        self.kind, self.mi, self.first, self.width, self.number = kind, mi, first, width, number


def planned(phases, chunks, ready):
    now, plan, tail = 0.0, {}, []
    free = {"S": 0.0, "R": 0.0, "L": 0.0}
    sets = {"g": [ZERO, ONE], "d": [ZERO]}
    state = {q: ["S0", None] for q in chunks}
    order = ["S0", "L1", "C1", "L2", "C2", "L3", "C3", "L4", "C4", "end"]
    load = 1.8

    def send(way, size, rate):
        free[way] = max(free[way], now) + size / rate
        return free[way] + 2.0

    def run(point):
        done = []
        again = True
        while again:
            again = False
            for q in chunks:
                stage, when = state[q]
                if stage == "end":
                    continue
                size = q.rows * q.width * TWO
                if stage == "S0":
                    if point is not None and point < ready[q]:
                        continue
                    if q.kind == "g":
                        done.append(("S0", q, ZERO))
                        state[q] = ["L1", send("S", 4 * size, 6e5)]
                    else:
                        state[q] = ["L1", now + 5]
                    again = True
                    continue
                if when > now:
                    continue
                if stage[ZERO] == "L":
                    if not sets[q.kind]:
                        continue
                    q.set = sets[q.kind].pop(ZERO)
                    done.append((stage, q, q.set))
                    state[q] = ["C" + stage[ONE], now + load]
                    again = True
                    continue
                sets[q.kind].append(q.set)
                done.append((stage, q, q.set))
                nxt = order[order.index(stage) + ONE]
                if stage == "C1":
                    when = max(send("R", size / TWO, 46600), send("L", size / TWO, 46600))
                elif stage == "C2":
                    q.right = send("R", size, 46600)
                    when = now
                elif stage == "C3":
                    when = max(q.right, send("L", size, 46600))
                state[q] = [nxt, when]
                again = True
        return done

    for p, (name, points, us) in enumerate(phases):
        for s in range(points):
            got = run((p, s))
            if got:
                plan[name, s] = got
            now += us + 0.3 * len(got)
    last = now
    while any(state[q][ZERO] != "end" for q in chunks):
        got = run(None)
        tail += got
        now += 0.5 + 0.3 * len(got)
    return plan, tail, last, now


CUTS = (5, 10, 14)


def bwd_kernel(n, dy, H1, WGT, WUT, WD, GATE, UP, HIDT, AT,
               GG, GU, GD, SQ, DG, DU, OWNg, Tg, ARg, X1g, X2g, OWNd, Td, ARd, X1d, X2d,
               dyv, sqv, og, ag, xg, yg, o1g, o2g, o3g, o4g, od, ad, xd, yd, o1d, o2d, o3d, o4d,
               slots, s0s, s0r, d0s, d0r, x1s, x1r, x2s, x2r, ld, fin, sems, one, ts, tr):
    T, D = dy.shape
    L, F, _ = WD.shape
    chips = n // TWO
    RG, RD = D // n, F // n
    full, rest = F // TN, F % TN
    r, me = lax.axis_index("rep"), lax.axis_index("dp")
    right, left = lax.rem(me + TWO, n), lax.rem(me + n - TWO, n)
    core = lax.rem(me, TWO)
    chip = lax.div(me, TWO)
    sib = me + ONE - TWO * core
    to = {"R": (r, right), "L": (r, left), "S": (r, sib)}
    at_chip = [lax.rem(chip + k, chips) for k in range(chips)]
    FAR = (chips // TWO, ONE, chips - ONE, ZERO)

    DI, GI = {"d1": ZERO, "d0": ONE}, {"g1": ZERO, "u1": ONE, "g0": TWO, "u0": 3}
    edges = [ZERO] + [k * TN for k in CUTS] + [F]
    last_step = [k - ONE for k in CUTS] + [full]
    chunks = []
    for pair in (("d1",), ("g1", "u1"), ("d0",), ("g0", "u0")):
        for c in range(TWO if pair[ZERO] in DI else len(edges) - ONE):
            for nm in pair:
                down = nm in DI
                a, w = (c * (D // TWO), D // TWO) if down else (edges[c], edges[c + ONE] - edges[c])
                q = Chunk("d" if down else "g", DI.get(nm, GI.get(nm)), a, w, c)
                q.rows, q.name = (RD if down else RG), nm
                q.half = (q.rows // 32 * 16, q.rows - q.rows // 32 * 16)
                chunks.append(q)
    nt = T // TB
    phases = [("d1", chips, 8.3), ("m1", TWO * full + TWO, 2.7), ("a1", nt * (D // TD), 3.4), ("d0", chips, 8.3), ("m0", TWO * full + TWO, 2.7)]
    index = {p[ZERO]: i for i, p in enumerate(phases)}
    ready = {}
    for q in chunks:
        if q.kind == "d":
            ready[q] = (index[q.name], TWO)
        elif last_step[q.number] == full:
            ready[q] = (index["m" + q.name[ONE]] + ONE, ZERO)
        else:
            ready[q] = (index["m" + q.name[ONE]], TWO * (last_step[q.number] + ONE) + ONE)
    plan, tail, _, _ = planned(phases, chunks, ready)

    refs = {"g": (OWNg, Tg, ARg, X1g, X2g, og, ag, xg, yg, (o1g, o2g, o3g, o4g)),
            "d": (OWNd, Td, ARd, X1d, X2d, od, ad, xd, yd, (o1d, o2d, o3d, o4d))}
    outs = {"g1": (GG, ONE), "u1": (GU, ONE), "d1": (GD, ONE), "g0": (GG, ZERO), "u0": (GU, ZERO), "d0": (GD, ZERO)}
    def remote(src, dst, ss, rs, way):
        return pltpu.make_async_remote_copy(src_ref=src, dst_ref=dst, send_sem=ss, recv_sem=rs, device_id=to[way], device_id_type=MESH)

    sent = []

    def cols_of(q): return pl.ds(q.first, q.width)

    def s0_copy(q):
        return remote(Tg.at[q.mi, :, :, cols_of(q)], ARg.at[q.mi, :, :, cols_of(q)], s0s.at[q.mi, q.number], s0r.at[q.mi, q.number], "S")

    def d0_copy(mi, i, where):
        return remote(Td.at[mi, where], ARd.at[mi, where], d0s.at[mi, i], d0r.at[mi, i], "S")

    def sem_of(q): return (q.mi if q.kind == "g" else 4 + q.mi), q.number

    slot, before, user = {}, {}, {}
    in_order = [e for name, points, _ in phases for s in range(points) for e in plan.get((name, s), ())] + tail
    for kind, q, _ in in_order:
        if kind[ZERO] == "C":
            key = (q.kind, int(kind[ONE]))
            k = len([p for p in slot if p[ONE] == key[ONE] and p[ZERO].kind == q.kind]) % refs[q.kind][9][ZERO].shape[ZERO]
            slot[q, key[ONE]], before[q, key[ONE]] = k, user.get(key + (k,))
            user[key + (k,)] = q

    def out_of(q, stage):
        return refs[q.kind][9][stage - ONE].at[slot[q, stage]]

    def result_copy(q):
        G, l = outs[q.name]
        k = slot[q, 4]
        return pltpu.make_async_copy(out_of(q, 4).at[:, pl.ds(ZERO, q.width)], G.at[l, :, cols_of(q)], fin.at[k if q.kind == "g" else TWO])

    def settle(q, stage):
        if q is None: return
        if stage == ONE:
            for half in (ZERO, ONE): x1_copy(q, half).wait_send()
        elif stage < 4:
            x2_copy(q, stage - TWO).wait_send()
        else:
            result_copy(q).wait()

    def x1_copy(q, half):
        X1, out = refs[q.kind][3], out_of(q, ONE)
        h = pl.ds(ZERO, q.half[half])
        a, c = sem_of(q)
        return remote(out.at[pl.ds(half * q.half[ZERO], q.half[half]), pl.ds(ZERO, q.width)], X1.at[q.mi, half, h, cols_of(q)], x1s.at[a, c, half], x1r.at[a, c, half], "RL"[half])

    def x2_copy(q, side):
        X2, out = refs[q.kind][4], out_of(q, TWO + side)
        a, c = sem_of(q)
        return remote(out.at[:, pl.ds(ZERO, q.width)], X2.at[q.mi, side, :, cols_of(q)], x2s.at[a, c, side], x2r.at[a, c, side], "RL"[side])

    def loads(stage, q, z):
        OWN, _, AR, X1, X2, vo, va, vx, vy, _ = refs[q.kind]
        vo, va, vx, vy = vo.at[z], va.at[z], vx.at[z], vy.at[z]
        where = at_chip[FAR[stage - ONE]]
        base = 4 * z if q.kind == "g" else 8
        h = q.half
        w = pl.ds(ZERO, q.width)
        got = [pltpu.make_async_copy(OWN.at[q.mi, where, :, cols_of(q)], vo.at[:, w], ld.at[base]),
               pltpu.make_async_copy(AR.at[q.mi, where, :, cols_of(q)], va.at[:, w], ld.at[base + ONE])]
        if stage == TWO:
            got.append(pltpu.make_async_copy(X1.at[q.mi, ZERO, pl.ds(ZERO, h[ZERO]), cols_of(q)], vx.at[pl.ds(ZERO, h[ZERO]), w], ld.at[base + TWO]))
        if stage == 3:
            got.append(pltpu.make_async_copy(X1.at[q.mi, ONE, pl.ds(ZERO, h[ONE]), cols_of(q)], vx.at[pl.ds(h[ZERO], h[ONE]), w], ld.at[base + TWO]))
        if stage == 4:
            got.append(pltpu.make_async_copy(X2.at[q.mi, ZERO, :, cols_of(q)], vx.at[:, w], ld.at[base + TWO]))
            got.append(pltpu.make_async_copy(X2.at[q.mi, ONE, :, cols_of(q)], vy.at[:, w], ld.at[base + 3]))
        return got

    STEP = {"g": 48, "d": 16}

    def event(kind, q, z):
        stage = int(kind[ONE])
        if kind == "S0":
            s0_copy(q).start()
            sent.append(lambda: s0_copy(q).wait_send())
            return
        vo, va, vx, vy = refs[q.kind][5:9]
        if kind[ZERO] == "L":
            if q.kind == "g":
                if stage == ONE: s0_copy(q).wait_recv()
            elif q.number == ZERO:
                d0_copy(q.mi, stage - ONE, at_chip[FAR[stage - ONE]]).wait_recv()
            if stage == TWO: x1_copy(q, ZERO).wait_recv()
            if stage == 3: x1_copy(q, ONE).wait_recv()
            if stage == 4:
                x2_copy(q, ZERO).wait_recv(); x2_copy(q, ONE).wait_recv()
            for c in loads(stage, q, z): c.start()
            return
        for c in loads(stage, q, z): c.wait()
        out, k = refs[q.kind][9][stage - ONE], slot[q, stage]
        settle(before[q, stage], stage)
        w, h = pl.ds(ZERO, q.width), q.half[ZERO]
        by = STEP[q.kind]

        def rows_loop(first, count, fn):
            def body(i, carry):
                fn(pl.ds(pl.multiple_of(first + i * by, 16), by))
                return carry
            lax.fori_loop(ZERO, count // by, body, ZERO)

        def plain(rows):
            out[k, rows, w] = (vo[z, rows, w] + va[z, rows, w].astype(F32)).astype(BF)
        def one_more(rows):
            out[k, rows, w] = (vo[z, rows, w] + va[z, rows, w].astype(F32) + vx[z, rows, w].astype(F32)).astype(BF)
        def final(rows):
            g = (vo[z, rows, w] + va[z, rows, w].astype(F32) + vx[z, rows, w].astype(F32) + vy[z, rows, w].astype(F32)).astype(BF)
            out[k, rows, w] = g
            g = g.astype(F32)
            g = g * g
            total = g[ZERO:8]
            for p in range(8, by, 8): total = total + g[p:p + 8]
            sqv[:, w] += total
        if stage == ONE:
            rows_loop(ZERO, q.rows, plain)
            for half in (ZERO, ONE): x1_copy(q, half).start()
        elif stage in (TWO, 3):
            rows_loop(ZERO, h, one_more if stage == TWO else plain); rows_loop(h, q.half[ONE], plain if stage == TWO else one_more)
            x2_copy(q, stage - TWO).start()
        else:
            rows_loop(ZERO, q.rows, final)
            result_copy(q).start()

    def events(name, j, steps, parity=None):
        for s in range(steps):
            if (name, s) in plan and parity in (None, s % TWO):
                @pl.when(j == s)
                def _():
                    for e in plan[name, s]: event(*e)

    def events_at(name, s):
        for e in plan.get((name, s), ()): event(*e)

    others = [lax.rem(me + k, n) for k in range(ONE, n)]
    barrier = pltpu.get_barrier_semaphore()
    for other in others:
        pl.semaphore_signal(barrier, inc=ONE, device_id=(r, other), device_id_type=MESH)
    pl.semaphore_wait(barrier, n - ONE)
    first = pltpu.make_async_copy(dy, dyv, one)
    first.start()
    sqv[...] = jnp.zeros_like(sqv)
    first.wait()

    def cols(j): return pl.ds(pl.multiple_of(j * TN, TN), TN)
    LAST = pl.ds(full * TN, rest)

    def far(i):
        k = jnp.where(i == ZERO, FAR[ZERO], jnp.where(i == ONE, FAR[ONE], jnp.where(i == TWO, FAR[TWO], FAR[3])))
        return lax.rem(chip + k, chips)

    def down_weights(name, l):
        mi = DI[name]
        def body(lhs, mb, tb):
            def rows(i, w): return pl.ds(pl.multiple_of((TWO * far(i) + (ONE - core if w == ZERO else core)) * RD, 8), RD)
            def l_in(i, w): return pltpu.make_async_copy(HIDT.at[l, rows(i, w)], lhs.at[w], sems.at[w])
            def t_out(i): return pltpu.make_async_copy(tb, Td.at[mi, far(i)], sems.at[TWO])
            def m_out(i): return pltpu.make_async_copy(mb, OWNd.at[mi, far(i)], sems.at[3])
            l_in(ZERO, ZERO).start(); l_in(ZERO, ONE).start()
            def step(i, carry):
                l_in(i, ZERO).wait()
                @pl.when(i > ZERO)
                def _():
                    t_out(i - ONE).wait()
                    d0_copy(mi, i - ONE, far(i - ONE)).start()
                tb[...] = jnp.dot(lhs[ZERO], dyv[...], preferred_element_type=F32).astype(BF)
                t_out(i).start()
                @pl.when(i + ONE < chips)
                def _(): l_in(i + ONE, ZERO).start()
                l_in(i, ONE).wait()
                @pl.when(i > ZERO)
                def _(): m_out(i - ONE).wait()
                events(name, i, chips)
                mb[...] = jnp.dot(lhs[ONE], dyv[...], preferred_element_type=F32)
                m_out(i).start()
                @pl.when(i + ONE < chips)
                def _(): l_in(i + ONE, ONE).start()
                return carry
            lax.fori_loop(ZERO, chips, step, ZERO)
            t_out(chips - ONE).wait()
            d0_copy(mi, chips - ONE, far(chips - ONE)).start()
            m_out(chips - ONE).wait()
            for i in range(chips): sent.append(lambda i=i: d0_copy(mi, i, at_chip[FAR[i]]).wait_send())
        pl.run_scoped(body, pltpu.VMEM((TWO, RD, T), BF), pltpu.VMEM((RD, D), F32), pltpu.VMEM((RD, D), BF))

    def hidden_and_weights(name, l):
        gi, ui = GI[f"g{l}"], GI[f"u{l}"]
        def body(av, wbuf, gbuf, ubuf, dgbuf, dubuf, fg, fu, bg, bu):
            a_in = pltpu.make_async_copy(AT.at[l], av, sems.at[ZERO])
            a_in.start()
            def size(j): return rest if isinstance(j, int) and j == full else TN
            def at(j): return LAST if isinstance(j, int) and j == full else cols(j)
            def ins(j, s):
                w = pl.ds(ZERO, size(j))
                return [pltpu.make_async_copy(WD.at[l, at(j)], wbuf.at[s, w], sems.at[ONE + s]),
                        pltpu.make_async_copy(GATE.at[l, j, :, w], gbuf.at[s, :, w], sems.at[3 + s]),
                        pltpu.make_async_copy(UP.at[l, j, :, w], ubuf.at[s, :, w], sems.at[5 + s])]
            def states_out(j, s):
                if not l: return []
                w = pl.ds(ZERO, size(j))
                return [pltpu.make_async_copy(dgbuf.at[s, :, w], DG.at[:, at(j)], sems.at[7 + s]),
                        pltpu.make_async_copy(dubuf.at[s, :, w], DU.at[:, at(j)], sems.at[9 + s])]
            def terms_out(j):
                w = pl.ds(ZERO, size(j))
                return [pltpu.make_async_copy(fg.at[:, core, :, w], OWNg.at[gi, :, :, at(j)], sems.at[11]),
                        pltpu.make_async_copy(bg.at[:, ONE - core, :, w], Tg.at[gi, :, :, at(j)], sems.at[12]),
                        pltpu.make_async_copy(fu.at[:, core, :, w], OWNg.at[ui, :, :, at(j)], sems.at[13]),
                        pltpu.make_async_copy(bu.at[:, ONE - core, :, w], Tg.at[ui, :, :, at(j)], sems.at[14])]
            def first_half(j, s):
                w = pl.ds(ZERO, size(j))
                turned = wbuf[s, w].T
                for c in range(T // CH):
                    rows = pl.ds(c * CH, CH)
                    by = jnp.dot(dyv[rows], turned, preferred_element_type=F32).astype(BF).astype(F32)
                    g = gbuf[s, rows, w]
                    sig = ONE / (ONE + jnp.exp(-g))
                    silu = g * sig
                    dubuf[s, rows, w] = (by * silu).astype(BF)
                    dgbuf[s, rows, w] = (by * ubuf[s, rows, w] * (sig + silu * (ONE - sig))).astype(BF)
            def second_half(j, s):
                w = pl.ds(ZERO, size(j))
                for rhs, f, b in ((dgbuf, fg, bg), (dubuf, fu, bu)):
                    for c in range(chips):
                        got = jnp.dot(av[pl.ds(c * TWO * RG, TWO * RG)], rhs[s, :, w], preferred_element_type=F32)
                        for k in (ZERO, ONE):
                            f[c, k, :, w] = got[k * RG:(k + ONE) * RG]
                            b[c, k, :, w] = got[k * RG:(k + ONE) * RG].astype(BF)
            for c in ins(ZERO, ZERO): c.start()
            a_in.wait()
            def step(j, carry):
                s = lax.rem(j, TWO)
                for c in ins(j, s): c.wait()
                @pl.when(j + ONE < full)
                def _():
                    for c in ins(j + ONE, ONE - s): c.start()
                @pl.when(j + ONE == full)
                def _():
                    for c in ins(full, full % TWO): c.start()
                if l:
                    @pl.when(j >= TWO)
                    def _():
                        for c in states_out(j - TWO, s): c.wait()
                events(name, TWO * j, TWO * full, ZERO)
                first_half(j, s)
                for c in states_out(j, s): c.start()
                @pl.when(j >= ONE)
                def _():
                    for c in terms_out(j - ONE): c.wait()
                events(name, TWO * j + ONE, TWO * full, ONE)
                second_half(j, s)
                for c in terms_out(j): c.start()
                return carry
            lax.fori_loop(ZERO, full, step, ZERO)
            s = full % TWO
            for c in ins(full, s): c.wait()
            for c in states_out(full - TWO, s): c.wait()
            events_at(name, TWO * full)
            first_half(full, s)
            for c in states_out(full, s): c.start()
            for c in terms_out(full - ONE): c.wait()
            events_at(name, TWO * full + ONE)
            second_half(full, s)
            for c in terms_out(full): c.start()
            for c in states_out(full - ONE, ONE - s) + states_out(full, s) + terms_out(full): c.wait()
        V = pltpu.VMEM
        pl.run_scoped(body, V((D, T), BF), V((TWO, TN, D), BF), V((TWO, T, TN), F32), V((TWO, T, TN), F32), V((TWO, T, TN), BF), V((TWO, T, TN), BF),
                      V((chips, TWO, RG, TN), F32), V((chips, TWO, RG, TN), F32), V((chips, TWO, RG, TN), BF), V((chips, TWO, RG, TN), BF))

    def states(name, l):
        nd = D // TD
        def body(lg, lu, rg, ru, dav, hv):
            def ins(t, s):
                rows = pl.ds(pl.multiple_of(t * TB, TB), TB)
                return [pltpu.make_async_copy(DG.at[rows], lg.at[s], sems.at[s]), pltpu.make_async_copy(DU.at[rows], lu.at[s], sems.at[TWO + s])]
            def w_in(d, s):
                return [pltpu.make_async_copy(WGT.at[d], rg.at[s], sems.at[4 + s]), pltpu.make_async_copy(WUT.at[d], ru.at[s], sems.at[6 + s])]
            def h_in(t): return pltpu.make_async_copy(H1.at[pl.ds(pl.multiple_of(t * TB, TB), TB)], hv, sems.at[8])
            for c in ins(ZERO, ZERO) + w_in(ZERO, ZERO): c.start()
            def step(q, carry):
                t, d = lax.div(q, nd), lax.rem(q, nd)
                s, p = lax.rem(t, TWO), lax.rem(q, TWO)
                @pl.when(d == ZERO)
                def _():
                    for c in ins(t, s): c.wait()
                    h_in(t).start()
                    @pl.when(t + ONE < nt)
                    def _():
                        for c in ins(t + ONE, ONE - s): c.start()
                for c in w_in(d, p): c.wait()
                @pl.when(q + ONE < nt * nd)
                def _():
                    for c in w_in(lax.rem(q + ONE, nd), ONE - p): c.start()
                events(name, q, nt * nd)
                a = jnp.dot(lg[s], rg[p], preferred_element_type=F32).astype(BF)
                b = jnp.dot(lu[s], ru[p], preferred_element_type=F32).astype(BF)
                dav[:, pl.ds(pl.multiple_of(d * TD, TD), TD)] = (a.astype(F32) + b.astype(F32)).astype(BF)
                @pl.when(d == nd - ONE)
                def _():
                    h_in(t).wait()
                    def rows_of(i, carry):
                        rr = pl.ds(pl.multiple_of(i * 64, 64), 64)
                        wide, by = hv[rr].astype(F32), dav[rr].astype(F32)
                        scale = lax.rsqrt(jnp.mean(wide * wide, -ONE, keepdims=True) + 1e-6)
                        inner = jnp.sum(by * wide, -ONE, keepdims=True) * (scale * scale * scale / D)
                        back = (by * scale - wide * inner).astype(BF)
                        here = pl.ds(pl.multiple_of(t * TB + i * 64, 64), 64)
                        dyv[here] = (dyv[here].astype(F32) + back.astype(F32)).astype(BF)
                        return carry
                    lax.fori_loop(ZERO, TB // 64, rows_of, ZERO)
                return carry
            lax.fori_loop(ZERO, nt * nd, step, ZERO)
        V = pltpu.VMEM
        pl.run_scoped(body, V((TWO, TB, F), BF), V((TWO, TB, F), BF), V((TWO, F, TD), BF), V((TWO, F, TD), BF), V((TB, D), BF), V((TB, D), BF))

    down_weights("d1", ONE)
    hidden_and_weights("m1", ONE)
    states("a1", ONE)
    down_weights("d0", ZERO)
    hidden_and_weights("m0", ZERO)
    for e in tail: event(*e)
    for (kind, stage, k), q in user.items(): settle(q, stage)
    slots[me] = jnp.full(slots.shape[ONE:], jnp.sum(sqv[...]), F32)
    def total_copy(k, whose):
        return pltpu.make_async_remote_copy(src_ref=slots.at[whose], dst_ref=slots.at[whose], send_sem=ts.at[k], recv_sem=tr.at[whose],
                                            device_id=(r, others[k]), device_id_type=MESH)
    for k in range(n - ONE): total_copy(k, me).start()
    for c in sent: c()
    for k in range(n - ONE): total_copy(k, others[k]).wait_recv()
    for k in range(n - ONE): total_copy(k, me).wait_send()
    total = slots[ZERO]
    for k in range(ONE, n): total = total + slots[k]
    sqv[ZERO:8, ZERO:128] = total
    put = pltpu.make_async_copy(sqv.at[ZERO:8, ZERO:128], SQ, one)
    put.start()
    put.wait()


def bwd(n, dy, H1, WGT, WUT, WD, GATE, UP, HIDT, AT):
    T, D = dy.shape
    L, F, _ = WD.shape
    RG, RD, chips = D // n, F // n, n // TWO
    edges = [ZERO] + [k * TN for k in CUTS] + [F]
    wide_g, wide_d = max(b - a for a, b in zip(edges, edges[ONE:])), D // TWO
    nc = len(CUTS) + ONE
    S = jax.ShapeDtypeStruct
    A = pl.BlockSpec(memory_space=pl.ANY)
    DMA, V = pltpu.SemaphoreType.DMA, pltpu.VMEM
    ng, nd = TWO * L, L
    def adds(R, w, k): return [V((k, R, w), F32), V((k, R, w), BF), V((k, R, w), BF), V((k, R, w), BF)] + [V((k, R, w), BF)] * 4
    return pl.pallas_call(
        functools.partial(bwd_kernel, n),
        out_shape=[S((L, RG, F), BF), S((L, RG, F), BF), S((L, RD, D), BF), S((8, 128), F32), S((T, F), BF), S((T, F), BF),
                   S((ng, chips, RG, F), F32), S((ng, chips, RG, F), BF), S((ng, chips, RG, F), BF), S((ng, TWO, RG - RG // 32 * 16, F), BF), S((ng, TWO, RG, F), BF),
                   S((nd, chips, RD, D), F32), S((nd, chips, RD, D), BF), S((nd, chips, RD, D), BF), S((nd, TWO, RD - RD // 32 * 16, D), BF), S((nd, TWO, RD, D), BF)],
        in_specs=[A] * 9, out_specs=[A] * 16,
        scratch_shapes=[V((T, D), BF), V((8, max(wide_g, wide_d)), F32)] + adds(RG, wide_g, TWO) + adds(RD, wide_d, ONE) + [V((n, 8, 128), F32),
            DMA((4, nc)), DMA((4, nc)), DMA((TWO, 4)), DMA((TWO, 4)), DMA((6, nc, TWO)), DMA((6, nc, TWO)), DMA((6, nc, TWO)), DMA((6, nc, TWO)),
            DMA((12,)), DMA((3,)), DMA((16,)), DMA(()), DMA((n - ONE,)), DMA((n,))],
        compiler_params=pltpu.CompilerParams(collective_id=ONE, has_side_effects=True, vmem_limit_bytes=VMEM_LIMIT),
        name="backward",
    )(dy, H1, WGT, WUT, WD, GATE, UP, HIDT, AT)[:4]


def adamw(w, m, v, g):
    m = 0.9 * m + 0.1 * g
    v = 0.95 * v + 0.05 * g * g
    step = m * lax.rsqrt(v + 1e-8) + 0.1 * w
    return (w - 0.02 * step).astype(BF), m, v


def solution(mesh):
    n = mesh.shape["dp"]

    def step(x, dy, *arrays):
        weights, m, v = (arrays[i : i + 3] for i in (ZERO, 3, 6))
        _, _, WD, GATE, UP, HIDT, AT, H1, WGT, WUT = fwd(n, x[ZERO], *weights)
        *gradients, squares = bwd(n, dy[ZERO], H1, WGT, WUT, WD, GATE, UP, HIDT, AT)
        count = lax.psum(ONE, "dp") * sum(g.size for g in gradients)
        factor = jnp.minimum(1.0, 0.5 * lax.rsqrt(squares[ZERO, ZERO] / count + 1e-30))
        new = [adamw(w.astype(F32), m, v, g.astype(F32) * factor) for w, m, v, g in zip(weights, m, v, gradients, strict=True)]
        return tuple(one[which] for which in range(3) for one in new)

    states, cut = P(("rep", "dp"), None, None), P(None, "dp", None)
    return jax.shard_map(step, mesh=mesh, in_specs=(states, states) + (cut,) * 9, out_specs=(P("rep", "dp", None),) * 9, check_vma=False)
```
